32 devices in a mesh: groups: 2 (over y), section: 4 (over z), tensor: 4 (over x, core).
Axes of the slice: x: 2, y: 2, z: 4, core: 2. Of those that a mesh axis runs over, the one named last changes fastest.
Arguments:
- images: bfloat16 [2, 32, 3072], P('groups', None, 'tensor'), parts along dimension 0, may hold values from -6 to 6
- w_qkv: bfloat16 [4, 3, 3072, 3072], P('section', None, None, 'tensor'), may hold values from -0.109375 to 0.109375
- qk_gain: float32 [4, 2, 3072], P('section', None, 'tensor'), may hold values from 0.1 to 1.9
- w_out: bfloat16 [4, 3072, 3072], P('section', None, 'tensor'), may hold values from -0.109375 to 0.109375
- in_gain: float32 [4, 3072], P('section'), may hold values from 0.1 to 1.9
- out_gain: float32 [3072], P('tensor'), may hold values from 0.1 to 1.9
Outputs:
- pooled: float32 [4, 2, 3072], P('section', 'groups', 'tensor'), parts along dimension 1
The draws below stay inside these ranges and needn't reach their ends.
There are 2 independent parts, one for each index of `groups`. The reference program is written for one: setup_inputs(seed, part) draws one part's arguments, and reference() takes and returns one part's arrays. A program takes and returns all parts, laid end to end along the dimension named above; an argument that names none is the same for every part. Nothing has to cross between parts.
All inputs are finite; a program needn't handle non-finite values.
Results may differ from the reference program's by a relative error of at most 0.015.
Values may be sent and summed in bfloat16 or wider, within the bound.
A program may use at most 64 MiB of HBM per device.

```python
import jax
import jax.numpy as jnp
from jax import lax

D = 3072
HEAD = 64
PATCHES = 32
MICRO = 1
INNER = 3072
LAYERS = 4
N_SECTION = 4


def steps_of(rng, shape, split, low, largest):
    loudness = 1.0
    for position, parts in split:
        heights = jax.random.uniform(jax.random.fold_in(jax.random.fold_in(rng, 6), position), (parts,), jnp.float32, low / len(split), largest / len(split))
        loudness = loudness * jnp.repeat(jnp.exp(heights), shape[position] // parts).reshape((-1,) + (1,) * (len(shape) - 1 - position))
    return loudness


def bell_draw(rng, shape, scale, bound, pieces=(), dtype=jnp.bfloat16):
    result = scale * jax.random.normal(rng, shape, jnp.float32)
    if pieces:
        result = result * steps_of(rng, shape, pieces, -0.22, 0.18)
    return jnp.clip(result, -bound, bound).astype(dtype)


def setup_inputs(seed: int = 0, part: int = 0) -> dict:
    seeds = jax.random.split(jax.random.key(seed), 7)
    own_keys = jax.random.split(jax.random.fold_in(seeds[6], part), 7)
    images = bell_draw(own_keys[0], (MICRO, PATCHES, D), 1.0, 6.0, ((2, 4),))
    w_qkv = bell_draw(seeds[1], (LAYERS, 3, D, INNER), D ** -0.5, 0.109375, ((0, 4), (3, 4)))
    qk_gain = jnp.clip(1.0 + 0.18 * jax.random.normal(seeds[2], (LAYERS, 2, INNER), jnp.float32), 0.1, 1.9)
    w_out = bell_draw(seeds[3], (LAYERS, INNER, D), INNER ** -0.5, 0.109375, ((0, 4), (2, 4)))
    in_gain = jnp.clip(1.0 + 0.18 * jax.random.normal(seeds[4], (LAYERS, D), jnp.float32), 0.1, 1.9)
    out_gain = jnp.clip(1.0 + 0.18 * jax.random.normal(seeds[5], (D,), jnp.float32), 0.1, 1.9)
    return {"images": images, "w_qkv": w_qkv, "qk_gain": qk_gain, "w_out": w_out, "in_gain": in_gain, "out_gain": out_gain}


def layer_norm(values, gain):
    centre = values - lax.optimization_barrier(jnp.mean(values, axis=-1, keepdims=True))
    spread = lax.optimization_barrier(jnp.mean(centre * centre, axis=-1, keepdims=True))
    return centre * lax.rsqrt(spread + 1e-06) * gain

def one_layer(state, weights, gains, outward, norm_gain):
    rows = state.shape[0]
    heads = weights.shape[2] // HEAD
    normed = layer_norm(state.astype(jnp.float32), norm_gain).astype(jnp.bfloat16)
    proj = jnp.einsum('td,cde->cte', normed.astype(jnp.float32), weights.astype(jnp.float32))
    query = layer_norm(proj[0].reshape(rows, heads, HEAD), gains[0].reshape(heads, HEAD)).astype(jnp.bfloat16)
    keys = layer_norm(proj[1].reshape(rows, heads, HEAD), gains[1].reshape(heads, HEAD)).astype(jnp.bfloat16)
    values = proj[2].astype(jnp.bfloat16).reshape(rows, heads, HEAD)
    scores = jnp.einsum('qhe,khe->hqk', query.astype(jnp.float32), keys.astype(jnp.float32)) * HEAD ** (-0.5)
    expo = jnp.exp(scores)
    probs = (expo / lax.optimization_barrier(jnp.sum(expo, axis=-1, keepdims=True))).astype(jnp.bfloat16)
    att = jnp.einsum('hqk,khe->qhe', probs.astype(jnp.float32), values.astype(jnp.float32))
    att = att.astype(jnp.bfloat16).reshape(rows, heads * HEAD)
    return (state.astype(jnp.float32) + jnp.dot(att, outward, preferred_element_type=jnp.float32)).astype(jnp.bfloat16)

def reference(images, w_qkv, qk_gain, w_out, in_gain, out_gain):
    per_layer = [[] for layer in range(N_SECTION)]
    for micro in range(images.shape[0]):
        state = images[micro]
        for layer in range(N_SECTION):
            state = one_layer(state, w_qkv[layer], qk_gain[layer], w_out[layer], in_gain[layer])
            average = lax.optimization_barrier(jnp.mean(state.astype(jnp.float32), axis=0))
            per_layer[layer].append(layer_norm(average, out_gain))
    return jnp.stack([jnp.stack(items) for items in per_layer])
```

```python
import functools

import jax
import jax.numpy as jnp
from jax import lax
from jax.experimental import pallas as pl
from jax.experimental.pallas import tpu as pltpu
from jax.sharding import PartitionSpec as P

HEAD = 64
EPS = 1e-06
MESH = pl.DeviceIdType.MESH


def remote(src, dst, send_sem, recv_sem, section, member):
    return pltpu.make_async_remote_copy(
        src_ref=src,
        dst_ref=dst,
        send_sem=send_sem,
        recv_sem=recv_sem,
        device_id={"section": section, "tensor": member},
        device_id_type=MESH,
    )


def block_mean(values, averager):
    high = values.astype(jnp.bfloat16)
    low = (values - high.astype(jnp.float32)).astype(jnp.bfloat16)
    return jnp.dot(high, averager, preferred_element_type=jnp.float32) + jnp.dot(
        low, averager, preferred_element_type=jnp.float32
    )


def kernel(
    sections,
    n,
    images,
    w_qkv,
    qk_gain,
    w_out,
    in_gain,
    pooled,
    wq,
    wo,
    gains,
    norm_gain,
    state,
    att,
    fresh,
    stats,
    w_sem,
    wo_sem,
    gain_sem,
    x_send,
    x_fwd,
    x_recv,
    a_send,
    a_fwd,
    a_recv,
    y_send,
    s_send,
    s_recv,
):
    section = lax.axis_index("section")
    me = lax.axis_index("tensor")
    chips = n // 2
    core = lax.rem(me, 2)
    chip = me // 2
    sibling = chip * 2 + 1 - core
    rows, span = fresh.shape
    inner = att.shape[2]
    width = n * span
    first = section == 0
    last = section == sections - 1

    def member_of(k):
        return lax.rem(chip + k, chips) * 2 + core

    image_copy = pltpu.make_async_copy(images.at[0], state.at[me], gain_sem.at[2])

    @pl.when(first)
    def _():
        image_copy.start()

    gain_copies = [
        pltpu.make_async_copy(in_gain, norm_gain, gain_sem.at[0]),
        pltpu.make_async_copy(qk_gain.at[0], gains, gain_sem.at[1]),
    ]
    for copy in gain_copies:
        copy.start()
    w_copies = [
        pltpu.make_async_copy(
            w_qkv.at[0, :, pl.ds(j * span, span), :], wq.at[:, pl.ds(j * span, span), :], w_sem.at[j]
        )
        for j in range(n)
    ]
    for copy in w_copies:
        copy.start()
    wo_copy = pltpu.make_async_copy(w_out.at[0], wo, wo_sem)
    wo_copy.start()

    barrier = pltpu.get_barrier_semaphore()
    for k in range(1, n):
        pl.semaphore_signal(
            barrier, inc=1, device_id={"section": section, "tensor": lax.rem(me + k, n)}, device_id_type=MESH
        )

    @pl.when(jnp.logical_not(first))
    def _():
        for k in range(chips):
            pl.semaphore_signal(
                barrier, inc=1, device_id={"section": section - 1, "tensor": member_of(k)}, device_id_type=MESH
            )

    @pl.when(jnp.logical_not(last))
    def _():
        for k in range(chips):
            pl.semaphore_signal(
                barrier, inc=1, device_id={"section": section + 1, "tensor": member_of(k)}, device_id_type=MESH
            )

    neighbours = (section > 0).astype(jnp.int32) + (section < sections - 1).astype(jnp.int32)
    pl.semaphore_wait(barrier, n - 1 + chips * neighbours)

    def outgoing(buffer, send, recv):
        copies = [
            remote(buffer.at[me], buffer.at[me], send.at[k], recv.at[me], section, member_of(k))
            for k in range(1, chips)
        ]
        copies.append(remote(buffer.at[me], buffer.at[me], send.at[0], recv.at[me], section, sibling))
        return copies

    def relay(buffer, fwd, recv, k):
        piece = member_of(k)
        return remote(buffer.at[piece], buffer.at[piece], fwd.at[k], recv.at[piece], section, sibling)

    def arrival(buffer, send, recv, piece):
        return remote(buffer.at[piece], buffer.at[piece], send.at[0], recv.at[piece], section, sibling)

    def gather(buffer, send, fwd, recv):
        for k in range(1, chips):
            arrival(buffer, send, recv, member_of(k)).wait_recv()
            relay(buffer, fwd, recv, k).start()
        for k in range(chips):
            arrival(buffer, send, recv, lax.rem(chip + k, chips) * 2 + 1 - core).wait_recv()

    @pl.when(first)
    def _():
        image_copy.wait()
        for copy in outgoing(state, x_send, x_recv):
            copy.start()
        gather(state, x_send, x_fwd, x_recv)

    @pl.when(jnp.logical_not(first))
    def _():
        for k in range(chips):
            arrival(state, x_send, x_recv, member_of(k)).wait_recv()
            relay(state, x_fwd, x_recv, k).start()
        for k in range(chips):
            arrival(state, x_send, x_recv, lax.rem(chip + k, chips) * 2 + 1 - core).wait_recv()

    for copy in gain_copies:
        copy.wait()

    pieces = [state[j].astype(jnp.float32) for j in range(n)]
    total = pieces[0].sum(axis=-1, keepdims=True)
    for j in range(1, n):
        total = total + pieces[j].sum(axis=-1, keepdims=True)
    mean = total * (1.0 / width)
    spread = jnp.zeros_like(mean)
    for j in range(n):
        centre = pieces[j] - mean
        spread = spread + (centre * centre).sum(axis=-1, keepdims=True)
    scale = lax.rsqrt(spread * (1.0 / width) + EPS)
    proj = [None, None, None]
    for j in range(n):
        gain = norm_gain[:, j * span : (j + 1) * span]
        normed = ((pieces[j] - mean) * scale * gain).astype(jnp.bfloat16)
        w_copies[j].wait()
        for c in range(3):
            part = jnp.dot(normed, wq[c, j * span : (j + 1) * span, :], preferred_element_type=jnp.float32)
            proj[c] = part if proj[c] is None else proj[c] + part

    block = 2 * HEAD if inner % (2 * HEAD) == 0 else HEAD
    blocks = inner // block
    pair = block // HEAD
    side_rows = lax.broadcasted_iota(jnp.int32, (block, block), 0) < HEAD
    side_columns = lax.broadcasted_iota(jnp.int32, (block, block), 1) < HEAD
    averager = jnp.where(side_rows == side_columns, 1.0 / HEAD, 0.0).astype(jnp.bfloat16)
    stacked = jnp.concatenate(
        [proj[c][:, b * block : (b + 1) * block] for c in range(2) for b in range(blocks)], axis=0
    )
    centre = stacked - block_mean(stacked, averager)
    factor = lax.rsqrt(block_mean(centre * centre, averager) + EPS)
    normal = centre * factor
    left = lax.broadcasted_iota(jnp.int32, (rows, block), 1) < HEAD
    scores = []
    for b in range(blocks):
        lanes = slice(b * block, (b + 1) * block)
        query = (normal[b * rows : (b + 1) * rows] * gains[0:1, lanes]).astype(jnp.bfloat16)
        at = (blocks + b) * rows
        keys = (normal[at : at + rows] * gains[1:2, lanes]).astype(jnp.bfloat16)
        if pair == 2:
            zero = jnp.zeros_like(query)
            query = jnp.concatenate([jnp.where(left, query, zero), jnp.where(left, zero, query)], axis=0)
        scores.append(
            lax.dot_general(query, keys, (((1,), (1,)), ((), ())), preferred_element_type=jnp.float32)
        )
    expo = jnp.exp(jnp.concatenate(scores, axis=0) * HEAD ** (-0.5))
    probs = (expo / jnp.sum(expo, axis=-1, keepdims=True)).astype(jnp.bfloat16)
    for b in range(blocks):
        lanes = slice(b * block, (b + 1) * block)
        values = proj[2][:, lanes].astype(jnp.bfloat16)
        mixed = jnp.dot(
            probs[b * pair * rows : (b + 1) * pair * rows], values, preferred_element_type=jnp.float32
        )
        if pair == 2:
            mixed = jnp.where(left, mixed[:rows], mixed[rows:])
        att[me, :, lanes] = mixed.astype(jnp.bfloat16)

    for copy in outgoing(att, a_send, a_recv):
        copy.start()
    gather(att, a_send, a_fwd, a_recv)
    wo_copy.wait()
    added = state[me].astype(jnp.float32)
    update = None
    for j in range(n):
        part = jnp.dot(att[j], wo[j * inner : (j + 1) * inner, :], preferred_element_type=jnp.float32)
        update = part if update is None else update + part
    whole = (added + update).astype(jnp.bfloat16)
    fresh[...] = whole

    def onward(k):
        return remote(fresh, state.at[me], y_send.at[k], x_recv.at[me], section + 1, member_of(k))

    @pl.when(jnp.logical_not(last))
    def _():
        for k in range(chips):
            onward((k + 1) % chips).start()

    average = jnp.sum(whole.astype(jnp.float32), axis=0, keepdims=True) * (1.0 / rows)
    local_mean = jnp.sum(average, axis=-1, keepdims=True) * (1.0 / span)
    off = average - local_mean
    local_spread = jnp.sum(off * off, axis=-1, keepdims=True)
    shape = stats.shape[2:]
    stats[me, 0] = jnp.broadcast_to(local_mean, shape)
    stats[me, 1] = jnp.broadcast_to(local_spread, shape)
    stat_copies = [
        remote(stats.at[me], stats.at[me], s_send.at[k], s_recv.at[me], section, lax.rem(me + k, n))
        for k in range(1, n)
    ]
    for copy in stat_copies:
        copy.start()
    for k in range(1, n):
        arrival(stats, s_send, s_recv, lax.rem(me + k, n)).wait_recv()
    centre_all = stats[0, 0]
    for j in range(1, n):
        centre_all = centre_all + stats[j, 0]
    centre_all = centre_all * (1.0 / n)
    spread_all = jnp.zeros(shape, jnp.float32)
    for j in range(n):
        gap = stats[j, 0] - centre_all
        spread_all = spread_all + (stats[j, 1] + span * (gap * gap))
    factor = lax.rsqrt(spread_all * (1.0 / width) + EPS)
    pooled[...] = (average - centre_all[0:1, 0:1]) * factor[0:1, 0:1]

    @pl.when(first)
    def _():
        for copy in outgoing(state, x_send, x_recv):
            copy.wait_send()

    @pl.when(jnp.logical_not(first))
    def _():
        relay(state, x_fwd, x_recv, 0).wait_send()

    for k in range(1, chips):
        relay(state, x_fwd, x_recv, k).wait_send()
        relay(att, a_fwd, a_recv, k).wait_send()
    for copy in outgoing(att, a_send, a_recv):
        copy.wait_send()
    for copy in stat_copies:
        copy.wait_send()

    @pl.when(jnp.logical_not(last))
    def _():
        for k in range(chips):
            onward(k).wait_send()


def solution(mesh):
    sections, n = mesh.shape["section"], mesh.shape["tensor"]

    def shards(images, w_qkv, qk_gain, w_out, in_gain, out_gain):
        rows, span = images.shape[1], images.shape[2]
        width, inner = w_qkv.shape[2], w_qkv.shape[3]
        dma = pltpu.SemaphoreType.DMA
        normal = pl.pallas_call(
            functools.partial(kernel, sections, n),
            out_shape=jax.ShapeDtypeStruct((1, span), jnp.float32),
            in_specs=[pl.BlockSpec(memory_space=pl.ANY)] * 5,
            out_specs=pl.BlockSpec(memory_space=pltpu.VMEM),
            scratch_shapes=[
                pltpu.VMEM((3, width, inner), jnp.bfloat16),
                pltpu.VMEM((w_out.shape[1], span), jnp.bfloat16),
                pltpu.VMEM((2, inner), jnp.float32),
                pltpu.VMEM((1, width), jnp.float32),
                pltpu.VMEM((n, rows, span), jnp.bfloat16),
                pltpu.VMEM((n, rows, inner), jnp.bfloat16),
                pltpu.VMEM((rows, span), jnp.bfloat16),
                pltpu.VMEM((n, 2, 8, 128), jnp.float32),
                dma((n,)),
                dma,
                dma((3,)),
                dma((n // 2,)),
                dma((n // 2,)),
                dma((n,)),
                dma((n // 2,)),
                dma((n // 2,)),
                dma((n,)),
                dma((n // 2,)),
                dma((n,)),
                dma((n,)),
            ],
            compiler_params=pltpu.CompilerParams(collective_id=0, has_side_effects=True),
        )(images, w_qkv, qk_gain, w_out, in_gain)
        return (normal * out_gain)[:, None, :]

    return jax.shard_map(
        shards,
        mesh=mesh,
        in_specs=(
            P("groups", None, "tensor"),
            P("section", None, None, "tensor"),
            P("section", None, "tensor"),
            P("section", None, "tensor"),
            P("section", None),
            P("tensor"),
        ),
        out_specs=P("section", "groups", "tensor"),
        check_vma=False,
    )
```
